32 devices in a mesh: dp: 8 (over z, x), ctx: 4 (over y, core).
Axes of the slice: x: 2, y: 2, z: 4, core: 2. Of those that a mesh axis runs over, the one named last changes fastest.
Arguments:
- tokens: bfloat16 [8, 512, 4096], P('dp', 'ctx'), may hold values from -6 to 6
- w_query: bfloat16 [4096, 512], P('dp', 'ctx'), may hold values from -0.09375 to 0.09375
- w_key: bfloat16 [4096, 512], P('dp', 'ctx'), may hold values from -0.09375 to 0.09375
- w_value: bfloat16 [4096, 1024], P('dp', 'ctx'), may hold values from -0.09375 to 0.09375
- decay_log: float32 [8, 2, 512], P('dp'), may hold values from -1 to 0, as said below
- group_gain: float32 [1024], P('ctx'), may hold values from 0.1 to 1.9
Outputs:
- retained: bfloat16 [8, 512, 1024], P('dp', 'ctx')
The draws below stay inside these ranges and needn't reach their ends.
Inputs may be any that keep to these rules, and one draw needn't show every extreme that they name: `decay_log`: every entry is negative.
All inputs are finite; a program needn't handle non-finite values.
Results may differ from the reference program's by a relative error of at most 0.0068.
Values may be sent and summed in bfloat16 or wider, within the bound.
No kernel may reach another device: no remote copies, remote signals or barrier semaphores. Data moves between devices by JAX's collectives and lax.ppermute only.
A program may use at most 64 MiB of HBM per device.

```python
import math
import jax
import jax.numpy as jnp
from jax import lax

D = 4096
KEY = 256
VAL = 512
BLOCK = 512
TOK_DEV = 128
RETENTION_HEADS = 2
SEQUENCE_LENGTH = 512
BATCH_SEQUENCES = 8


def draw_decay_log(key, part):
    random_subkeys = jax.random.split(key, 7)
    fast_share = 0.5
    head_shape = (BATCH_SEQUENCES, RETENTION_HEADS, 1)
    is_fast = jax.random.uniform(random_subkeys[0], head_shape) < fast_share
    fast_rate = jnp.exp(jax.random.uniform(random_subkeys[1], head_shape, minval=math.log(1.0 / 50.0), maxval=math.log(1.0 / 30.0)))
    slow_rate = jnp.exp(jax.random.uniform(random_subkeys[2], head_shape, minval=math.log(0.1 / SEQUENCE_LENGTH), maxval=math.log(0.3 / SEQUENCE_LENGTH)))
    baseline_rate = jnp.where(is_fast, fast_rate, slow_rate)
    block_count = SEQUENCE_LENGTH // TOK_DEV
    block_multiplier = jnp.exp(jax.random.uniform(random_subkeys[3], (BATCH_SEQUENCES, RETENTION_HEADS, block_count), minval=math.log(0.5), maxval=math.log(2.0)))
    block_multiplier = jnp.repeat(block_multiplier, TOK_DEV, axis=2)
    jaggedness = jax.random.uniform(random_subkeys[4], (BATCH_SEQUENCES, RETENTION_HEADS, SEQUENCE_LENGTH), minval=0.5, maxval=1.5)
    spike_mask = jax.random.uniform(random_subkeys[5], (BATCH_SEQUENCES, 1, SEQUENCE_LENGTH)) < 3.0 / SEQUENCE_LENGTH
    spike_loss = jnp.log(jax.random.uniform(random_subkeys[6], (BATCH_SEQUENCES, RETENTION_HEADS, SEQUENCE_LENGTH), minval=0.5, maxval=0.8))
    final_output = -(baseline_rate * block_multiplier * jaggedness) + jnp.where(spike_mask, spike_loss, 0.0)
    return final_output.astype(jnp.float32)


def shard_levels(stream_key, dims, cuts, least, largest):
    def one(dim, parts):
        heights = jax.random.uniform(jax.random.fold_in(jax.random.fold_in(stream_key, 6), dim), (parts,), jnp.float32, least / len(cuts), largest / len(cuts))
        return jnp.repeat(jnp.exp(heights), dims[dim] // parts).reshape((-1,) + (1,) * (len(dims) - dim - 1))

    factor_of = one(*cuts[0])
    for cut in cuts[1:]:
        factor_of = factor_of * one(*cut)
    return factor_of


def bell_draw(own_key, shape, scale, limit, cuts=(), held_as=jnp.bfloat16):
    array = scale * jax.random.normal(own_key, shape, jnp.float32)
    if cuts:
        array = array * shard_levels(own_key, shape, cuts, -0.22, 0.18)
    return jnp.clip(array, -limit, limit).astype(held_as)


def setup_inputs(seed: int = 0) -> dict:
    splits = jax.random.split(jax.random.key(seed), 7)
    tokens = bell_draw(splits[0], (BATCH_SEQUENCES, SEQUENCE_LENGTH, D), 1.0, 6.0, ((0, 8), (1, 4)))
    w_query = bell_draw(splits[1], (D, RETENTION_HEADS * KEY), D ** -0.5, 0.09375, ((0, 8), (1, 4)))
    w_key = bell_draw(splits[2], (D, RETENTION_HEADS * KEY), D ** -0.5, 0.09375, ((0, 8), (1, 4)))
    w_value = bell_draw(splits[3], (D, RETENTION_HEADS * VAL), D ** -0.5, 0.09375, ((0, 8), (1, 4)))
    decay_log = draw_decay_log(jax.random.fold_in(splits[6], 71), 0)
    group_gain = jnp.clip(1.0 + 0.18 * jax.random.normal(splits[5], (RETENTION_HEADS * VAL,), jnp.float32), 0.1, 1.9)
    return {"tokens": tokens, "w_query": w_query, "w_key": w_key, "w_value": w_value, "decay_log": decay_log, "group_gain": group_gain}


norm_eps = 1e-05

def retain(query, keys, values, decay):
    length = query.shape[0]
    blocks = length // BLOCK
    scaling = query.shape[1] ** (-0.5)
    summed = jnp.cumsum(decay)
    q_blocks = query.reshape(blocks, BLOCK, query.shape[1])
    k_blocks = keys.reshape(blocks, BLOCK, keys.shape[1])
    v_blocks = values.reshape(blocks, BLOCK, values.shape[1])
    a_blocks = summed.reshape(blocks, BLOCK)
    row_ids = lax.broadcasted_iota(jnp.int32, (BLOCK, BLOCK), 0)
    col_ids = lax.broadcasted_iota(jnp.int32, (BLOCK, BLOCK), 1)
    causal = row_ids >= col_ids

    def advance(carried_in, pieces):
        memory, prior_log = carried_in
        q_block, k_block, v_block, a_block = pieces
        scores = jnp.dot(q_block, k_block.T, preferred_element_type=jnp.float32) * scaling
        spread_log = jnp.where(causal, a_block[:, None] - a_block[None, :], 0.0)
        weights = jnp.where(causal, scores * jnp.exp(spread_log), 0.0).astype(jnp.bfloat16)
        inside = jnp.dot(weights, v_block, preferred_element_type=jnp.float32)
        lead_query = q_block.astype(jnp.float32) * (scaling * jnp.exp(a_block - prior_log))[:, None]
        carried = jnp.dot(lead_query, memory, precision=lax.Precision.HIGHEST, preferred_element_type=jnp.float32)
        last_log = a_block[-1]
        faded_keys = k_block.astype(jnp.float32) * jnp.exp(last_log - a_block)[:, None]
        memory = jnp.exp(last_log - prior_log) * memory + jnp.dot(faded_keys.T, v_block.astype(jnp.float32), precision=lax.Precision.HIGHEST, preferred_element_type=jnp.float32)
        return ((memory, last_log), inside + carried)
    start_carry = (jnp.zeros((query.shape[1], values.shape[1]), jnp.float32), jnp.zeros((), jnp.float32))
    _, outputs = lax.scan(advance, start_carry, (q_blocks, k_blocks, v_blocks, a_blocks))
    return outputs.reshape(length, values.shape[1])

def reference(tokens, w_query, w_key, w_value, decay_log, group_gain):

    def one_sequence(paired):
        sequence, rates = paired
        length = sequence.shape[0]
        heads = rates.shape[0]
        query = jnp.dot(sequence, w_query, preferred_element_type=jnp.float32).astype(jnp.bfloat16)
        keys = jnp.dot(sequence, w_key, preferred_element_type=jnp.float32).astype(jnp.bfloat16)
        values = jnp.dot(sequence, w_value, preferred_element_type=jnp.float32).astype(jnp.bfloat16)
        q_heads = query.reshape(length, heads, KEY).transpose(1, 0, 2)
        k_heads = keys.reshape(length, heads, KEY).transpose(1, 0, 2)
        v_heads = values.reshape(length, heads, VAL).transpose(1, 0, 2)
        outputs = lax.map(lambda group: retain(group[0], group[1], group[2], group[3]), (q_heads, k_heads, v_heads, rates))
        average = lax.optimization_barrier(jnp.mean(outputs, axis=2, keepdims=True))
        centered = outputs - average
        spread = lax.optimization_barrier(jnp.mean(centered * centered, axis=2, keepdims=True))
        normed = centered * lax.rsqrt(spread + norm_eps)
        normed = normed.transpose(1, 0, 2).reshape(length, heads * VAL)
        return (normed * group_gain[None, :]).astype(jnp.bfloat16)
    return lax.map(one_sequence, (tokens, decay_log))
```

```python
import math

import jax
import jax.numpy as jnp
from jax import lax
from jax.sharding import PartitionSpec as P


BLOCK = 512
norm_eps = 1e-05
TOKEN_MOST = 6.0
WEIGHT_MOST = 0.09375


def flipped(value, axis, mask):
    pairs = [(source, source ^ mask) for source in range(lax.axis_size(axis))]
    return lax.ppermute(value, axis, pairs)


def flipped_both(value, mask_dp, mask_ctx):
    ctx = lax.axis_size("ctx")
    pairs = [
        (source, ((source // ctx) ^ mask_dp) * ctx + ((source % ctx) ^ mask_ctx))
        for source in range(lax.axis_size("dp") * ctx)
    ]
    return lax.ppermute(value, ("dp", "ctx"), pairs)


def place_at(turn, count):
    return jnp.where(turn <= count // 2, jnp.maximum(2 * turn - 1, 0), 2 * (count - turn))


def turn_of(place, count):
    half = (place + 1) // 2
    return jnp.where(place % 2 == 1, half, jnp.where(place == 0, 0, count - half))


def loop_order(count):
    return [0] + list(range(1, count, 2)) + list(range(2, count, 2))[::-1]


def columns_of(tokens, outer, width, parity):
    return jnp.concatenate(
        [
            lax.dynamic_slice_in_dim(tokens, (2 * step + parity) * width, width, axis=1)
            for step in range(outer)
        ],
        axis=1,
    )


def dot32(left, right):
    return jnp.dot(left, right, preferred_element_type=jnp.float32)


def dot_exact(left, right):
    return jnp.dot(
        left, right, precision=lax.Precision.HIGHEST, preferred_element_type=jnp.float32
    )


def retain(query, keys, values, summed, me, chunk):
    length = query.shape[0]
    blocks = length // BLOCK
    per_block = BLOCK // chunk
    scaling = query.shape[1] ** (-0.5)
    low = me % per_block
    high = me // per_block
    places = jnp.arange(per_block) ^ low
    pos = (places[:, None] * chunk + jnp.arange(chunk)[None, :]).reshape(BLOCK)
    causal = pos[:, None] >= pos[None, :]
    memory = jnp.zeros((query.shape[1], values.shape[1]), jnp.float32)
    prior_log = jnp.zeros((), jnp.float32)
    outputs = jnp.zeros((length, values.shape[1]), jnp.float32)
    for block in range(blocks):
        natural = summed[block * BLOCK : (block + 1) * BLOCK]
        if blocks == 1:
            q_block, k_block, v_block = query, keys, values
        else:
            start = (block ^ high) * BLOCK
            q_block = lax.dynamic_slice_in_dim(query, start, BLOCK, axis=0)
            k_block = lax.dynamic_slice_in_dim(keys, start, BLOCK, axis=0)
            v_block = lax.dynamic_slice_in_dim(values, start, BLOCK, axis=0)
        pieces = natural.reshape(per_block, chunk)
        a_block = jnp.concatenate(
            [
                lax.dynamic_index_in_dim(pieces, low ^ m, 0, keepdims=False)
                for m in range(per_block)
            ]
        )
        scores = dot32(q_block, k_block.T) * scaling
        spread_log = jnp.where(causal, a_block[:, None] - a_block[None, :], 0.0)
        weights = jnp.where(causal, scores * jnp.exp(spread_log), 0.0).astype(jnp.bfloat16)
        inside = dot32(weights, v_block)
        lead_query = q_block.astype(jnp.float32) * (scaling * jnp.exp(a_block - prior_log))[:, None]
        carried = dot_exact(lead_query, memory)
        last_log = natural[-1]
        faded_keys = k_block.astype(jnp.float32) * jnp.exp(last_log - a_block)[:, None]
        memory = jnp.exp(last_log - prior_log) * memory + dot_exact(
            faded_keys.T, v_block.astype(jnp.float32)
        )
        prior_log = last_log
        result = inside + carried
        if blocks == 1:
            outputs = result
        else:
            outputs = lax.dynamic_update_slice_in_dim(outputs, result, start, axis=0)
    return outputs


def whole(tokens, w_query, w_key, w_value, decay_log, group_gain):
    dp = lax.axis_size("dp")
    ctx = lax.axis_size("ctx")
    outer = dp // 2
    chunk = tokens.shape[1]
    width = w_query.shape[0]
    key_part = w_query.shape[1]
    rank = lax.axis_index("dp")
    me = lax.axis_index("ctx")
    parity = rank % 2
    turn = turn_of(rank // 2, outer)
    mine = tokens[0]

    order = loop_order(outer)
    ring = [
        (order[i] * 2 + p, order[(i + 1) % outer] * 2 + p) for i in range(outer) for p in range(2)
    ]
    held = [jnp.concatenate([w_query, w_key], axis=1), w_value]
    stages = [held]
    for _ in range(1, outer):
        sent = []
        for piece in held:
            sent.append(lax.ppermute(piece, "dp", ring))
        held = sent
        stages.append(held)
    sources = [place_at((turn + outer - step) % outer, outer) for step in range(outer)]

    own_tokens = columns_of(mine, outer, width, parity)
    away_tokens = columns_of(mine, outer, width, 1 - parity)

    def rows_of(piece, mask_dp):
        pieces = {}
        for m in range(0, ctx, 2):
            if m == 0 and mask_dp == 0:
                pieces[m] = piece
            else:
                pieces[m] = flipped_both(piece, mask_dp, m)
        for m in range(0, ctx, 2):
            pieces[m + 1] = flipped(pieces[m], "ctx", 1)
        rows = jnp.zeros((ctx * chunk, outer * width), piece.dtype)
        for m in range(ctx):
            rows = lax.dynamic_update_slice_in_dim(rows, pieces[m], m * chunk, axis=0)
        return rows

    own_rows = rows_of(own_tokens, 0)
    other_rows = rows_of(away_tokens, 1)

    def project(rows, part):
        total = None
        for step in range(outer):
            piece = lax.dynamic_slice_in_dim(rows, sources[step] * width, width, axis=1)
            product = dot32(piece, stages[step][part])
            total = product if total is None else total + product
        return total

    limit = TOKEN_MOST * WEIGHT_MOST * outer * width
    scale = 2.0 ** math.floor(math.log2(65504.0 / limit))

    def summed_over_pair(part):
        away = (project(other_rows, part) * scale).astype(jnp.float16)
        kept = project(own_rows, part)
        came = flipped(away, "dp", 1)
        return (kept + came.astype(jnp.float32) * (1.0 / scale)).astype(jnp.bfloat16)

    pair_mine = summed_over_pair(0)
    values = summed_over_pair(1)

    chunks = [pair_mine[m * chunk : (m + 1) * chunk] for m in range(ctx)]
    pair_other = flipped(jnp.concatenate([chunks[m ^ 1] for m in range(ctx)]), "ctx", 1)
    query = jnp.concatenate([pair_mine[:, :key_part], pair_other[:, :key_part]], axis=1)
    keys = jnp.concatenate([pair_mine[:, key_part:], pair_other[:, key_part:]], axis=1)

    rates = lax.dynamic_index_in_dim(decay_log[0], me // 2, 0, keepdims=False)
    outputs = retain(query, keys, values, jnp.cumsum(rates), me, chunk)

    count = outputs.shape[1]
    own_mean = jnp.mean(outputs, axis=1)
    own_squares = jnp.sum((outputs - own_mean[:, None]) ** 2, axis=1)
    stats = jnp.stack([own_mean, own_squares]).reshape(2, ctx // 2, 2, chunk)
    other = flipped(stats[:, :, ::-1], "ctx", 1).reshape(2, -1)
    average = 0.5 * (own_mean + other[0])
    squares = own_squares + other[1]
    squares = squares + count * ((own_mean - average) ** 2 + (other[0] - average) ** 2)
    spread = squares / (2 * count)
    centered = outputs - average[:, None]
    normed = (centered * lax.rsqrt(spread + norm_eps)[:, None] * group_gain[None, :]).astype(
        jnp.bfloat16
    )

    back = [normed[:chunk]]
    for m in range(1, ctx):
        back.append(flipped(normed[m * chunk : (m + 1) * chunk], "ctx", m))
    for bit in [1 << b for b in range(ctx.bit_length() - 1)]:
        swap = (me & bit) != 0
        back = [jnp.where(swap, back[m ^ bit], back[m]) for m in range(ctx)]
    return jnp.concatenate(back, axis=1)[None]


def solution(mesh):
    in_specs = (
        P("dp", "ctx", None),
        P("dp", "ctx"),
        P("dp", "ctx"),
        P("dp", "ctx"),
        P("dp", None, None),
        P("ctx"),
    )
    out_specs = P("dp", "ctx", None)
    return jax.shard_map(whole, mesh=mesh, in_specs=in_specs, out_specs=out_specs, check_vma=False)
```

```python
import math

import jax
import jax.numpy as jnp
from jax import lax
from jax.experimental import pallas as pl
from jax.experimental.pallas import tpu as pltpu
from jax.sharding import PartitionSpec as P


BLOCK = 512
norm_eps = 1e-05
TOKEN_MOST = 6.0
WEIGHT_MOST = 0.09375
GRANT = 16 * 2**20


def flipped(value, axis, mask):
    pairs = [(source, source ^ mask) for source in range(lax.axis_size(axis))]
    return lax.ppermute(value, axis, pairs)


def flipped_both(value, mask_dp, mask_ctx):
    ctx = lax.axis_size("ctx")
    pairs = [
        (source, ((source // ctx) ^ mask_dp) * ctx + ((source % ctx) ^ mask_ctx))
        for source in range(lax.axis_size("dp") * ctx)
    ]
    return lax.ppermute(value, ("dp", "ctx"), pairs)


def place_at(turn, count):
    return jnp.where(turn <= count // 2, jnp.maximum(2 * turn - 1, 0), 2 * (count - turn))


def turn_of(place, count):
    half = (place + 1) // 2
    return jnp.where(place % 2 == 1, half, jnp.where(place == 0, 0, count - half))


def loop_order(count):
    return [0] + list(range(1, count, 2)) + list(range(2, count, 2))[::-1]


def dot32(left, right):
    return jnp.dot(left, right, preferred_element_type=jnp.float32)


def dot_exact(left, right):
    return jnp.dot(
        left, right, precision=lax.Precision.HIGHEST, preferred_element_type=jnp.float32
    )


def near(operands):
    return [pltpu.with_memory_space_constraint(operand, pltpu.VMEM) for operand in operands]


def kernel(body, out, operands, scalars=None, scratch=(), far=()):
    vmem = pl.BlockSpec(memory_space=pltpu.VMEM)
    specs = [vmem] * len(operands) + [pl.BlockSpec(memory_space=pl.ANY)] * len(far)
    inputs = near(operands)
    inputs += [pltpu.with_memory_space_constraint(operand, pltpu.HBM) for operand in far]
    if scalars is not None:
        specs = [pl.BlockSpec(memory_space=pltpu.SMEM)] + specs
        inputs = [scalars] + inputs
    return pl.pallas_call(
        body,
        out_shape=out,
        in_specs=specs,
        out_specs=jax.tree.map(lambda _: vmem, out),
        scratch_shapes=list(scratch),
        compiler_params=pltpu.CompilerParams(vmem_limit_bytes=GRANT),
    )(*inputs)


def prepared(ids, tokens, w_query, w_key, outer):
    chunk = tokens.shape[0]
    width, part = w_query.shape

    def body(ids_ref, tokens_ref, query_ref, key_ref, pair_ref, own_ref, away_ref, arrivals):
        parity = ids_ref[0] % 2
        copies = [
            (query_ref, pair_ref.at[:, pl.ds(0, part)]),
            (key_ref, pair_ref.at[:, pl.ds(part, part)]),
        ]
        for step in range(outer):
            for side, out_ref in ((1 - parity, away_ref), (parity, own_ref)):
                start = pl.multiple_of((2 * step + side) * width, width)
                copies.append((tokens_ref.at[:, pl.ds(start, width)], out_ref.at[step]))
        copies = [
            pltpu.make_async_copy(source, target, arrivals.at[i])
            for i, (source, target) in enumerate(copies)
        ]
        for copy in copies:
            copy.start()
        for copy in copies:
            copy.wait()

    return kernel(
        body,
        [
            pltpu.VMEM((width, 2 * part), jnp.bfloat16),
            pltpu.VMEM((outer, chunk, width), jnp.bfloat16),
            pltpu.VMEM((outer, chunk, width), jnp.bfloat16),
        ],
        [],
        scalars=ids,
        scratch=[pltpu.SemaphoreType.DMA((2 + 2 * outer,))],
        far=[tokens, w_query, w_key],
    )


def decayed(ids, decay_log, chunk):
    _, length = decay_log.shape
    blocks = length // BLOCK
    per_block = BLOCK // chunk

    def body(ids_ref, rates_ref, row_ref, col_ref, end_ref, place_row, place_col, sums):
        head = ids_ref[1] // 2
        rates = rates_ref[pl.ds(head, 1), :]
        pieces = [rates[:, i * chunk : (i + 1) * chunk] for i in range(length // chunk)]
        before = lax.broadcasted_iota(jnp.int32, (chunk, chunk), 0)
        after = lax.broadcasted_iota(jnp.int32, (chunk, chunk), 1)
        inside = dot_exact(
            jnp.concatenate(pieces, axis=0), (before <= after).astype(jnp.float32)
        )
        carried = jnp.zeros((1, 1), jnp.float32)
        for i in range(length // chunk):
            sums[i : i + 1, :] = inside[i : i + 1, :] + carried
            carried = carried + inside[i : i + 1, chunk - 1 : chunk]
            if (i + 1) % per_block == 0:
                n = i // per_block
                end_ref[n : n + 1, :] = carried
        low = ids_ref[1] % per_block
        steps = lax.broadcasted_iota(jnp.int32, (1, chunk), 1)
        places = jnp.concatenate([(low ^ m) * chunk + steps for m in range(per_block)], axis=1)
        place_row[...] = places

        def column(row):
            return jnp.broadcast_to(row, (8, BLOCK)).T[:, :1]

        place_col[...] = column(places.astype(jnp.float32)).astype(jnp.int32)
        for n in range(blocks):
            row = jnp.concatenate(
                [sums[pl.ds(n * per_block + (low ^ m), 1), :] for m in range(per_block)], axis=1
            )
            row_ref[n] = row
            col_ref[n] = column(row)

    return kernel(
        body,
        [
            pltpu.VMEM((blocks, 1, BLOCK), jnp.float32),
            pltpu.VMEM((blocks, BLOCK, 1), jnp.float32),
            pltpu.VMEM((blocks, 1), jnp.float32),
            pltpu.VMEM((1, BLOCK), jnp.int32),
            pltpu.VMEM((BLOCK, 1), jnp.int32),
        ],
        [decay_log],
        scalars=ids,
        scratch=[pltpu.VMEM((length // chunk, chunk), jnp.float32)],
    )


def halved(weight):
    width, wide = weight.shape
    half = wide // 2

    def body(ref, first, second):
        first[...] = ref[:, :half]
        second[...] = ref[:, half:]

    return kernel(body, [pltpu.VMEM((width, half), weight.dtype)] * 2, [weight])


def mixed(ids, sides, stages):
    steps = len(stages)
    count = len(sides[0])
    _, chunk, width = sides[0][0].shape
    parts = [w.shape[1] for w in stages[0]]
    cuts = [sum(parts[:i]) for i in range(len(parts))]
    length = count * chunk

    def body(ids_ref, *refs):
        turn = turn_of(ids_ref[0] // 2, steps + 1)
        sources = [place_at((turn + steps + 1 - step) % (steps + 1), steps + 1) for step in range(steps + 1)]
        at = 0
        pieces = []
        for _ in sides:
            pieces.append(refs[at : at + count])
            at += count
        weights = []
        for _ in range(steps):
            weights.append(refs[at : at + len(parts)])
            at += len(parts)
        for side in pieces:
            total_ref, last = refs[at : at + 2]
            at += 2
            for m in range(0, count, 2):

                def rows(step):
                    return jnp.concatenate(
                        [side[m][sources[step]], side[m + 1][sources[step]]], axis=0
                    )

                span = pl.ds(m * chunk, 2 * chunk)
                for part, cut in zip(range(len(parts)), cuts):
                    total = None
                    for step in range(steps):
                        product = dot32(rows(step), weights[step][part][...])
                        total = product if total is None else total + product
                    total_ref[span, cut : cut + parts[part]] = total
                last[span, :] = rows(steps)

    outs = kernel(
        body,
        [
            pltpu.VMEM((length, sum(parts)), jnp.float32),
            pltpu.VMEM((length, width), jnp.bfloat16),
        ]
        * len(sides),
        [piece for side in sides for piece in side] + [w for step in stages for w in step],
        scalars=ids,
    )
    return outs[:2], outs[2:]


def projected(away, kept, weight, cut, scale):
    (length, _), part = away[0].shape, weight.shape[1]

    def body(away_total, away_last, kept_total, kept_last, w, away_out, kept_out):
        columns = w[...]
        span = slice(cut, cut + part)
        gone = away_total[:, span] + dot32(away_last[...], columns)
        away_out[...] = gone * scale
        kept_out[...] = kept_total[:, span] + dot32(kept_last[...], columns)

    return kernel(body, [pltpu.VMEM((length, part), jnp.float32)] * 2, [*away, *kept, weight])


def joined(kept, came, scale):
    return (kept + came.astype(jnp.float32) * (1.0 / scale)).astype(jnp.bfloat16)


def weighed(pair_mine, pair_other, decays, prior, memories):
    log_row, log_col, place_row, place_col = decays
    length, wide = pair_mine.shape
    part = wide // 2
    scaling = (2 * part) ** (-0.5)

    def body(mine, other, log_row, log_col, place_row, place_col, prior, *refs):
        states = refs[: len(memories)]
        out = refs[len(memories)]
        reads = refs[len(memories) + 1 :]

        def scored(ref, rows):
            return lax.dot_general(
                ref[rows, :part],
                ref[:, part:],
                (((1,), (1,)), ((), ())),
                preferred_element_type=jnp.float32,
            )

        tile = min(256, length)
        for start in range(0, length, tile):
            rows = pl.ds(start, tile)
            scores = (scored(mine, rows) + scored(other, rows)) * scaling
            causal = place_col[rows, :] >= place_row[...]
            spread_log = jnp.where(causal, log_col[rows, :] - log_row[...], 0.0)
            out[rows, :] = jnp.where(causal, scores * jnp.exp(spread_log), 0.0).astype(
                jnp.bfloat16
            )
            fade = scaling * jnp.exp(log_col[rows, :] - prior[...])
            for state, read in zip(states, reads):
                total = jnp.zeros((tile, state.shape[1]), jnp.float32)
                for i, ref in enumerate((mine, other)):
                    lead = ref[rows, :part].astype(jnp.float32) * fade
                    total = total + dot_exact(lead, state[i * part : (i + 1) * part, :])
                read[rows, :] = total

    outs = kernel(
        body,
        [pltpu.VMEM((length, length), jnp.bfloat16)]
        + [pltpu.VMEM((length, state.shape[1]), jnp.float32) for state in memories],
        [pair_mine, pair_other, log_row, log_col, place_row, place_col, prior, *memories],
    )
    return outs[0], outs[1:]


def applied(weights, values, carried, chunk):
    length, part = values.shape

    def body(weights_ref, values_ref, carried_ref, *outs):
        for m, out in enumerate(outs):
            rows = pl.ds(m * chunk, chunk)
            out[...] = dot32(weights_ref[rows, :], values_ref[...]) + carried_ref[rows, :]

    return kernel(
        body,
        [pltpu.VMEM((chunk, part), jnp.float32)] * (length // chunk),
        [weights, values, carried],
    )


def finished(ids, pieces, gains):
    count = len(pieces)
    groups = len(pieces[0])
    chunk, part = pieces[0][0].shape
    wide = groups * part

    def body(ids_ref, *refs):
        out = refs[-1]
        gain_refs = refs[count * groups : count * groups + count]
        for m in range(0, count, 2):
            mine = [refs[i] for i in range(m * groups, (m + 2) * groups)]
            total = sum(jnp.sum(ref[...], axis=1, keepdims=True) for ref in mine)
            average = total / (2 * wide)
            centered = [ref[...] - average for ref in mine]
            squares = sum(jnp.sum(c * c, axis=1, keepdims=True) for c in centered)
            rate = lax.rsqrt(squares / (2 * wide) + norm_eps)
            for i, c in enumerate(centered):
                which = m + i // groups
                group = i % groups
                gain = gain_refs[which][:, group * part : (group + 1) * part]
                start = pl.multiple_of((ids_ref[1] ^ which) * wide + group * part, part)
                out[:, pl.ds(start, part)] = (c * rate * gain).astype(jnp.bfloat16)

    return kernel(
        body,
        jax.ShapeDtypeStruct((chunk, count * wide), jnp.bfloat16),
        [ref for piece in pieces for ref in piece] + list(gains),
        scalars=ids,
    )


def whole(tokens, w_query, w_key, w_value, decay_log, group_gain):
    dp = lax.axis_size("dp")
    ctx = lax.axis_size("ctx")
    outer = dp // 2
    chunk = tokens.shape[1]
    width = w_query.shape[0]
    key_part = w_query.shape[1]
    half = w_value.shape[1] // 2
    rank = lax.axis_index("dp")
    me = lax.axis_index("ctx")
    ids = jnp.stack([rank, me]).astype(jnp.int32)
    length = ctx * chunk
    blocks = length // BLOCK
    high = me // (BLOCK // chunk)

    pair, own_tokens, away_tokens = prepared(ids, tokens[0], w_query, w_key, outer)
    log_rows, log_cols, ends, place_row, place_col = decayed(ids, decay_log[0], chunk)

    order = loop_order(outer)
    ring = [
        (order[i] * 2 + p, order[(i + 1) % outer] * 2 + p) for i in range(outer) for p in range(2)
    ]
    held = [pair, w_value]
    stages = []
    for step in range(1, outer):
        stages.append(held)
        if step == outer - 1:
            held = [held[0], *halved(held[1])]
        sent = []
        for piece in held:
            sent.append(lax.ppermute(piece, "dp", ring))
        held = sent

    def rows_of(piece, mask_dp):
        pieces = {}
        for m in range(0, ctx, 2):
            if m == 0 and mask_dp == 0:
                pieces[m] = piece
            else:
                pieces[m] = flipped_both(piece, mask_dp, m)
        for m in range(0, ctx, 2):
            pieces[m + 1] = flipped(pieces[m], "ctx", 1)
        return [pieces[m] for m in range(ctx)]

    own_rows = rows_of(own_tokens, 0)
    away_rows = rows_of(away_tokens, 1)
    gains = [group_gain[None]]
    for m in range(1, ctx):
        gains.append(flipped(group_gain[None], "ctx", m))

    away, kept = mixed(ids, (away_rows, own_rows), stages)

    limit = TOKEN_MOST * WEIGHT_MOST * outer * width
    scale = 2.0 ** math.floor(math.log2(65504.0 / limit))
    stays = []
    cut = 0
    for weight in held:
        gone, stay = projected(away, kept, weight, cut, scale)
        cut += weight.shape[1]
        stays.append((stay, flipped(gone.astype(jnp.float16), "dp", 1)))

    pair_mine = joined(*stays[0], scale)
    chunks = [pair_mine[m * chunk : (m + 1) * chunk] for m in range(ctx)]
    pair_other = flipped(jnp.concatenate([chunks[m ^ 1] for m in range(ctx)]), "ctx", 1)

    def cut_rows(array, block):
        if blocks == 1:
            return array
        return lax.dynamic_slice_in_dim(array, (block ^ high) * BLOCK, BLOCK, axis=0)

    memories = [jnp.zeros((2 * key_part, half), jnp.float32) for _ in stays[1:]]
    prior = jnp.zeros((1, 1), jnp.float32)
    outputs = [jnp.zeros((length, half), jnp.float32) for _ in stays[1:]]
    arrived = [[] for _ in range(ctx)]
    values = []
    for stay in stays[1:]:
        values.append(joined(*stay, scale))
    for n in range(blocks):
        mine, other = cut_rows(pair_mine, n), cut_rows(pair_other, n)
        decays = (log_rows[n], log_cols[n], place_row, place_col)
        weights, carried = weighed(mine, other, decays, prior, memories)
        k_block = jnp.concatenate([mine[:, key_part:], other[:, key_part:]], axis=1)
        end = ends[n : n + 1]
        faded = k_block.astype(jnp.float32) * jnp.exp(end - log_cols[n])
        for group in range(len(values)):
            v_block = cut_rows(values[group], n)
            results = applied(weights, v_block, carried[group], chunk)
            memories[group] = jnp.exp(end - prior) * memories[group] + dot_exact(
                faded.T, v_block.astype(jnp.float32)
            )
            if blocks > 1:
                outputs[group] = lax.dynamic_update_slice_in_dim(
                    outputs[group], jnp.concatenate(results), (n ^ high) * BLOCK, axis=0
                )
            else:
                outputs[group] = results
        prior = end
    for results in outputs:
        if blocks > 1:
            results = [results[m * chunk : (m + 1) * chunk] for m in range(ctx)]
        arrived[0].append(results[0])
        for m in range(1, ctx):
            arrived[m].append(flipped(results[m], "ctx", m))
    return finished(ids, arrived, gains)[None]


def solution(mesh):
    in_specs = (
        P("dp", "ctx", None),
        P("dp", "ctx"),
        P("dp", "ctx"),
        P("dp", "ctx"),
        P("dp", None, None),
        P("ctx"),
    )
    out_specs = P("dp", "ctx", None)
    return jax.shard_map(whole, mesh=mesh, in_specs=in_specs, out_specs=out_specs, check_vma=False)
```

```python
import math

import jax
import jax.numpy as jnp
from jax import lax
from jax.experimental import pallas as pl
from jax.experimental.pallas import tpu as pltpu
from jax.sharding import PartitionSpec as P


BLOCK = 512
norm_eps = 1e-05
TOKEN_MOST = 6.0
WEIGHT_MOST = 0.09375
GRANT = 16 * 2**20


def flipped(value, axis, mask):
    pairs = [(source, source ^ mask) for source in range(lax.axis_size(axis))]
    return lax.ppermute(value, axis, pairs)


def flipped_both(value, mask_dp, mask_ctx):
    ctx = lax.axis_size("ctx")
    pairs = [
        (source, ((source // ctx) ^ mask_dp) * ctx + ((source % ctx) ^ mask_ctx))
        for source in range(lax.axis_size("dp") * ctx)
    ]
    return lax.ppermute(value, ("dp", "ctx"), pairs)


def place_at(turn, count):
    return jnp.where(turn <= count // 2, jnp.maximum(2 * turn - 1, 0), 2 * (count - turn))


def turn_of(place, count):
    half = (place + 1) // 2
    return jnp.where(place % 2 == 1, half, jnp.where(place == 0, 0, count - half))


def loop_order(count):
    return [0] + list(range(1, count, 2)) + list(range(2, count, 2))[::-1]


def dot32(left, right):
    return jnp.dot(left, right, preferred_element_type=jnp.float32)


def dot_exact(left, right):
    return jnp.dot(
        left, right, precision=lax.Precision.HIGHEST, preferred_element_type=jnp.float32
    )


def near(operands):
    return [pltpu.with_memory_space_constraint(operand, pltpu.VMEM) for operand in operands]


def kernel(body, out, operands, scalars=None, scratch=(), far=()):
    vmem = pl.BlockSpec(memory_space=pltpu.VMEM)
    specs = [vmem] * len(operands) + [pl.BlockSpec(memory_space=pl.ANY)] * len(far)
    inputs = near(operands)
    inputs += [pltpu.with_memory_space_constraint(operand, pltpu.HBM) for operand in far]
    if scalars is not None:
        specs = [pl.BlockSpec(memory_space=pltpu.SMEM)] + specs
        inputs = [scalars] + inputs
    return pl.pallas_call(
        body,
        out_shape=out,
        in_specs=specs,
        out_specs=jax.tree.map(lambda _: vmem, out),
        scratch_shapes=list(scratch),
        compiler_params=pltpu.CompilerParams(vmem_limit_bytes=GRANT),
    )(*inputs)


def prepared(ids, tokens, w_query, w_key, outer):
    chunk = tokens.shape[0]
    width, part = w_query.shape

    def body(ids_ref, tokens_ref, query_ref, key_ref, pair_ref, own_ref, away_ref, arrivals):
        parity = ids_ref[0] % 2
        copies = [
            (query_ref, pair_ref.at[:, pl.ds(0, part)]),
            (key_ref, pair_ref.at[:, pl.ds(part, part)]),
        ]
        for step in range(outer):
            for side, out_ref in ((1 - parity, away_ref), (parity, own_ref)):
                start = pl.multiple_of((2 * step + side) * width, width)
                copies.append((tokens_ref.at[:, pl.ds(start, width)], out_ref.at[step]))
        copies = [
            pltpu.make_async_copy(source, target, arrivals.at[i])
            for i, (source, target) in enumerate(copies)
        ]
        for copy in copies:
            copy.start()
        for copy in copies:
            copy.wait()

    return kernel(
        body,
        [
            pltpu.VMEM((width, 2 * part), jnp.bfloat16),
            pltpu.VMEM((outer, chunk, width), jnp.bfloat16),
            pltpu.VMEM((outer, chunk, width), jnp.bfloat16),
        ],
        [],
        scalars=ids,
        scratch=[pltpu.SemaphoreType.DMA((2 + 2 * outer,))],
        far=[tokens, w_query, w_key],
    )


def decayed(ids, decay_log, chunk):
    _, length = decay_log.shape
    blocks = length // BLOCK
    per_block = BLOCK // chunk

    def body(ids_ref, rates_ref, row_ref, col_ref, end_ref, place_row, place_col, sums):
        head = ids_ref[1] // 2
        rates = rates_ref[pl.ds(head, 1), :]
        pieces = [rates[:, i * chunk : (i + 1) * chunk] for i in range(length // chunk)]
        before = lax.broadcasted_iota(jnp.int32, (chunk, chunk), 0)
        after = lax.broadcasted_iota(jnp.int32, (chunk, chunk), 1)
        inside = dot_exact(
            jnp.concatenate(pieces, axis=0), (before <= after).astype(jnp.float32)
        )
        carried = jnp.zeros((1, 1), jnp.float32)
        for i in range(length // chunk):
            sums[i : i + 1, :] = inside[i : i + 1, :] + carried
            carried = carried + inside[i : i + 1, chunk - 1 : chunk]
            if (i + 1) % per_block == 0:
                n = i // per_block
                end_ref[n : n + 1, :] = carried
        low = ids_ref[1] % per_block
        steps = lax.broadcasted_iota(jnp.int32, (1, chunk), 1)
        places = jnp.concatenate([(low ^ m) * chunk + steps for m in range(per_block)], axis=1)
        place_row[...] = places

        def column(row):
            return jnp.broadcast_to(row, (8, BLOCK)).T[:, :1]

        place_col[...] = column(places.astype(jnp.float32)).astype(jnp.int32)
        for n in range(blocks):
            row = jnp.concatenate(
                [sums[pl.ds(n * per_block + (low ^ m), 1), :] for m in range(per_block)], axis=1
            )
            row_ref[n] = row
            col_ref[n] = column(row)

    return kernel(
        body,
        [
            pltpu.VMEM((blocks, 1, BLOCK), jnp.float32),
            pltpu.VMEM((blocks, BLOCK, 1), jnp.float32),
            pltpu.VMEM((blocks, 1), jnp.float32),
            pltpu.VMEM((1, BLOCK), jnp.int32),
            pltpu.VMEM((BLOCK, 1), jnp.int32),
        ],
        [decay_log],
        scalars=ids,
        scratch=[pltpu.VMEM((length // chunk, chunk), jnp.float32)],
    )


def halved(weight):
    width, wide = weight.shape
    half = wide // 2

    def body(ref, first, second):
        first[...] = ref[:, :half]
        second[...] = ref[:, half:]

    return kernel(body, [pltpu.VMEM((width, half), weight.dtype)] * 2, [weight])


def mixed(ids, side, stages):
    steps = len(stages)
    count = len(side)
    _, chunk, width = side[0].shape
    parts = [w.shape[1] for w in stages[0]]
    cuts = [sum(parts[:i]) for i in range(len(parts))]
    length = count * chunk

    def body(ids_ref, *refs):
        turn = turn_of(ids_ref[0] // 2, steps + 1)
        sources = [place_at((turn + steps + 1 - step) % (steps + 1), steps + 1) for step in range(steps + 1)]
        total_ref, last = refs[-2:]
        pieces = refs[:count]
        weights = [
            refs[count + step * len(parts) : count + (step + 1) * len(parts)]
            for step in range(steps)
        ]
        for m in range(0, count, 2):

            def rows(step):
                return jnp.concatenate(
                    [pieces[m][sources[step]], pieces[m + 1][sources[step]]], axis=0
                )

            span = pl.ds(m * chunk, 2 * chunk)
            for part, cut in enumerate(cuts):
                total = None
                for step in range(steps):
                    product = dot32(rows(step), weights[step][part][...])
                    total = product if total is None else total + product
                total_ref[span, cut : cut + parts[part]] = total
            last[span, :] = rows(steps)

    return kernel(
        body,
        [
            pltpu.VMEM((length, sum(parts)), jnp.float32),
            pltpu.VMEM((length, width), jnp.bfloat16),
        ],
        list(side) + [w for step in stages for w in step],
        scalars=ids,
    )


def projected(side, weight, cut, factor):
    (length, _), part = side[0].shape, weight.shape[1]

    def body(total, last, w, out):
        out[...] = (total[:, cut : cut + part] + dot32(last[...], w[...])) * factor

    return kernel(body, pltpu.VMEM((length, part), jnp.float32), [*side, weight])


def joined(kept, came, scale):
    return (kept + came.astype(jnp.float32) * (1.0 / scale)).astype(jnp.bfloat16)


def weighed(pair_mine, pair_other, decays, prior, memories):
    log_row, log_col, place_row, place_col = decays
    length, wide = pair_mine.shape
    part = wide // 2
    scaling = (2 * part) ** (-0.5)

    def body(mine, other, log_row, log_col, place_row, place_col, prior, *refs):
        states = refs[: len(memories)]
        out = refs[len(memories)]
        reads = refs[len(memories) + 1 :]

        def scored(ref, rows):
            return lax.dot_general(
                ref[rows, :part],
                ref[:, part:],
                (((1,), (1,)), ((), ())),
                preferred_element_type=jnp.float32,
            )

        tile = min(256, length)
        for start in range(0, length, tile):
            rows = pl.ds(start, tile)
            scores = (scored(mine, rows) + scored(other, rows)) * scaling
            causal = place_col[rows, :] >= place_row[...]
            spread_log = jnp.where(causal, log_col[rows, :] - log_row[...], 0.0)
            out[rows, :] = jnp.where(causal, scores * jnp.exp(spread_log), 0.0).astype(
                jnp.bfloat16
            )
            fade = scaling * jnp.exp(log_col[rows, :] - prior[...])
            for state, read in zip(states, reads):
                total = jnp.zeros((tile, state.shape[1]), jnp.float32)
                for i, ref in enumerate((mine, other)):
                    lead = ref[rows, :part].astype(jnp.float32) * fade
                    total = total + dot_exact(lead, state[i * part : (i + 1) * part, :])
                read[rows, :] = total

    outs = kernel(
        body,
        [pltpu.VMEM((length, length), jnp.bfloat16)]
        + [pltpu.VMEM((length, state.shape[1]), jnp.float32) for state in memories],
        [pair_mine, pair_other, log_row, log_col, place_row, place_col, prior, *memories],
    )
    return outs[0], outs[1:]


def applied(weights, values, carried, chunk):
    length, part = values.shape

    def body(weights_ref, values_ref, carried_ref, *outs):
        for m, out in enumerate(outs):
            rows = pl.ds(m * chunk, chunk)
            out[...] = dot32(weights_ref[rows, :], values_ref[...]) + carried_ref[rows, :]

    return kernel(
        body,
        [pltpu.VMEM((chunk, part), jnp.float32)] * (length // chunk),
        [weights, values, carried],
    )


def finished(ids, pieces, gains):
    count = len(pieces)
    groups = len(pieces[0])
    chunk, part = pieces[0][0].shape
    wide = groups * part

    def body(ids_ref, *refs):
        out = refs[-1]
        gain_refs = refs[count * groups : count * groups + count]
        for m in range(0, count, 2):
            mine = [refs[i] for i in range(m * groups, (m + 2) * groups)]
            total = jnp.sum(sum(ref[...] for ref in mine), axis=1, keepdims=True)
            average = total / (2 * wide)
            centered = [ref[...] - average for ref in mine]
            squares = jnp.sum(sum(c * c for c in centered), axis=1, keepdims=True)
            rate = lax.rsqrt(squares / (2 * wide) + norm_eps)
            for i, c in enumerate(centered):
                which = m + i // groups
                group = i % groups
                gain = gain_refs[which][:, group * part : (group + 1) * part]
                start = pl.multiple_of((ids_ref[1] ^ which) * wide + group * part, part)
                out[:, pl.ds(start, part)] = (c * rate * gain).astype(jnp.bfloat16)

    return kernel(
        body,
        jax.ShapeDtypeStruct((chunk, count * wide), jnp.bfloat16),
        [ref for piece in pieces for ref in piece] + list(gains),
        scalars=ids,
    )


def whole(tokens, w_query, w_key, w_value, decay_log, group_gain):
    dp = lax.axis_size("dp")
    ctx = lax.axis_size("ctx")
    outer = dp // 2
    chunk = tokens.shape[1]
    width = w_query.shape[0]
    key_part = w_query.shape[1]
    half = w_value.shape[1] // 2
    rank = lax.axis_index("dp")
    me = lax.axis_index("ctx")
    ids = jnp.stack([rank, me]).astype(jnp.int32)
    length = ctx * chunk
    blocks = length // BLOCK
    high = me // (BLOCK // chunk)

    pair, own_tokens, away_tokens = prepared(ids, tokens[0], w_query, w_key, outer)
    log_rows, log_cols, ends, place_row, place_col = decayed(ids, decay_log[0], chunk)

    order = loop_order(outer)
    ring = [
        (order[i] * 2 + p, order[(i + 1) % outer] * 2 + p) for i in range(outer) for p in range(2)
    ]
    held = [pair, w_value]
    stages = []
    for step in range(1, outer):
        stages.append(held)
        if step == outer - 1:
            held = [held[0], *halved(held[1])]
        sent = []
        for piece in held:
            sent.append(lax.ppermute(piece, "dp", ring))
        held = sent

    def rows_of(piece, mask_dp):
        pieces = {}
        for m in range(0, ctx, 2):
            if m == 0 and mask_dp == 0:
                pieces[m] = piece
            else:
                pieces[m] = flipped_both(piece, mask_dp, m)
        for m in range(0, ctx, 2):
            pieces[m + 1] = flipped(pieces[m], "ctx", 1)
        return [pieces[m] for m in range(ctx)]

    own_rows = rows_of(own_tokens, 0)
    away_rows = rows_of(away_tokens, 1)
    gains = [group_gain[None]]
    for m in range(1, ctx):
        gains.append(flipped(group_gain[None], "ctx", m))

    away = mixed(ids, away_rows, stages)
    kept = mixed(ids, own_rows, stages)

    limit = TOKEN_MOST * WEIGHT_MOST * outer * width
    scale = 2.0 ** math.floor(math.log2(65504.0 / limit))
    stays = []
    cut = 0
    for weight in held:
        gone = projected(away, weight, cut, scale)
        stay = projected(kept, weight, cut, 1.0)
        cut += weight.shape[1]
        stays.append((stay, flipped(gone.astype(jnp.float16), "dp", 1)))

    pair_mine = joined(*stays[0], scale)
    chunks = [pair_mine[m * chunk : (m + 1) * chunk] for m in range(ctx)]
    pair_other = flipped(jnp.concatenate([chunks[m ^ 1] for m in range(ctx)]), "ctx", 1)

    def cut_rows(array, block):
        if blocks == 1:
            return array
        return lax.dynamic_slice_in_dim(array, (block ^ high) * BLOCK, BLOCK, axis=0)

    memories = [jnp.zeros((2 * key_part, half), jnp.float32) for _ in stays[1:]]
    prior = jnp.zeros((1, 1), jnp.float32)
    outputs = [jnp.zeros((length, half), jnp.float32) for _ in stays[1:]]
    arrived = [[] for _ in range(ctx)]
    values = []
    for stay in stays[1:]:
        values.append(joined(*stay, scale))
    for n in range(blocks):
        mine, other = cut_rows(pair_mine, n), cut_rows(pair_other, n)
        decays = (log_rows[n], log_cols[n], place_row, place_col)
        weights, carried = weighed(mine, other, decays, prior, memories)
        k_block = jnp.concatenate([mine[:, key_part:], other[:, key_part:]], axis=1)
        end = ends[n : n + 1]
        faded = k_block.astype(jnp.float32) * jnp.exp(end - log_cols[n])
        for group in range(len(values)):
            v_block = cut_rows(values[group], n)
            results = applied(weights, v_block, carried[group], chunk)
            memories[group] = jnp.exp(end - prior) * memories[group] + dot_exact(
                faded.T, v_block.astype(jnp.float32)
            )
            if blocks > 1:
                outputs[group] = lax.dynamic_update_slice_in_dim(
                    outputs[group], jnp.concatenate(results), (n ^ high) * BLOCK, axis=0
                )
            else:
                outputs[group] = results
        prior = end
    for results in outputs:
        if blocks > 1:
            results = [results[m * chunk : (m + 1) * chunk] for m in range(ctx)]
        arrived[0].append(results[0])
        for m in range(1, ctx):
            arrived[m].append(flipped(results[m], "ctx", m))
    return finished(ids, arrived, gains)[None]


def solution(mesh):
    in_specs = (
        P("dp", "ctx", None),
        P("dp", "ctx"),
        P("dp", "ctx"),
        P("dp", "ctx"),
        P("dp", None, None),
        P("ctx"),
    )
    out_specs = P("dp", "ctx", None)
    return jax.shard_map(whole, mesh=mesh, in_specs=in_specs, out_specs=out_specs, check_vma=False)
```

```python
import math

import jax
import jax.numpy as jnp
from jax import lax
from jax.experimental import pallas as pl
from jax.experimental.pallas import tpu as pltpu
from jax.sharding import PartitionSpec as P


BLOCK = 512
norm_eps = 1e-05
TOKEN_MOST = 6.0
WEIGHT_MOST = 0.09375
GRANT = 16 * 2**20
TAIL = 8


def flipped(value, axis, mask):
    pairs = [(source, source ^ mask) for source in range(lax.axis_size(axis))]
    return lax.ppermute(value, axis, pairs)


def place_at(turn, count):
    return jnp.where(turn <= count // 2, jnp.maximum(2 * turn - 1, 0), 2 * (count - turn))


def turn_of(place, count):
    half = (place + 1) // 2
    return jnp.where(place % 2 == 1, half, jnp.where(place == 0, 0, count - half))


def loop_order(count):
    return [0] + list(range(1, count, 2)) + list(range(2, count, 2))[::-1]


def dot32(left, right):
    return jnp.dot(left, right, preferred_element_type=jnp.float32)


def dot_exact(left, right):
    return jnp.dot(
        left, right, precision=lax.Precision.HIGHEST, preferred_element_type=jnp.float32
    )


def near(operands):
    return [pltpu.with_memory_space_constraint(operand, pltpu.VMEM) for operand in operands]


def kernel(body, out, operands, scalars=None, scratch=(), far=()):
    vmem = pl.BlockSpec(memory_space=pltpu.VMEM)
    specs = [vmem] * len(operands) + [pl.BlockSpec(memory_space=pl.ANY)] * len(far)
    inputs = near(operands)
    inputs += [pltpu.with_memory_space_constraint(operand, pltpu.HBM) for operand in far]
    if scalars is not None:
        specs = [pl.BlockSpec(memory_space=pltpu.SMEM)] + specs
        inputs = [scalars] + inputs
    return pl.pallas_call(
        body,
        out_shape=out,
        in_specs=specs,
        out_specs=jax.tree.map(lambda _: vmem, out),
        scratch_shapes=list(scratch),
        compiler_params=pltpu.CompilerParams(vmem_limit_bytes=GRANT),
    )(*inputs)


def prepared(ids, tokens, w_query, w_key, w_value, outer):
    chunk = tokens.shape[0] // 2
    width, part = w_query.shape
    half = w_value.shape[1] // 2

    def body(ids_ref, tokens_ref, query_ref, key_ref, value_ref, *refs):
        pair_ref, first_ref, second_ref = refs[:3]
        sides = (refs[3:5], refs[5:7])
        arrivals = refs[7]
        parity = ids_ref[0] % 2
        copies = [
            (query_ref, pair_ref.at[:, pl.ds(0, part)]),
            (key_ref, pair_ref.at[:, pl.ds(part, part)]),
        ]
        for side, outs in ((1 - parity, sides[0]), (parity, sides[1])):
            for i, out_ref in enumerate(outs):
                for step in range(outer):
                    start = pl.multiple_of((2 * step + side) * width, width)
                    source = tokens_ref.at[pl.ds(i * chunk, chunk), pl.ds(start, width)]
                    copies.append((source, out_ref.at[step]))
        copies += [
            (value_ref.at[:, pl.ds(0, half)], first_ref),
            (value_ref.at[:, pl.ds(half, half)], second_ref),
        ]
        copies = [
            pltpu.make_async_copy(source, target, arrivals.at[i])
            for i, (source, target) in enumerate(copies)
        ]
        for copy in copies:
            copy.start()
        for copy in copies:
            copy.wait()

    outs = kernel(
        body,
        [pltpu.VMEM((width, 2 * part), jnp.bfloat16)]
        + [pltpu.VMEM((width, half), jnp.bfloat16)] * 2
        + [pltpu.VMEM((outer, chunk, width), jnp.bfloat16)] * 4,
        [],
        scalars=ids,
        scratch=[pltpu.SemaphoreType.DMA((4 + 4 * outer,))],
        far=[tokens, w_query, w_key, w_value],
    )
    return outs[:3], outs[3:5], outs[5:]


def decayed(ids, decay_log, chunk):
    _, length = decay_log.shape
    blocks = length // BLOCK
    per_block = BLOCK // chunk

    def body(ids_ref, rates_ref, row_ref, col_ref, end_ref, place_row, place_col, sums):
        head = ids_ref[1] // 2
        rates = rates_ref[pl.ds(head, 1), :]
        pieces = [rates[:, i * chunk : (i + 1) * chunk] for i in range(length // chunk)]
        before = lax.broadcasted_iota(jnp.int32, (chunk, chunk), 0)
        after = lax.broadcasted_iota(jnp.int32, (chunk, chunk), 1)
        inside = dot_exact(
            jnp.concatenate(pieces, axis=0), (before <= after).astype(jnp.float32)
        )
        carried = jnp.zeros((1, 1), jnp.float32)
        for i in range(length // chunk):
            sums[i : i + 1, :] = inside[i : i + 1, :] + carried
            carried = carried + inside[i : i + 1, chunk - 1 : chunk]
            if (i + 1) % per_block == 0:
                n = i // per_block
                end_ref[n : n + 1, :] = carried
        low = ids_ref[1] % per_block
        steps = lax.broadcasted_iota(jnp.int32, (1, chunk), 1)
        places = jnp.concatenate([(low ^ m) * chunk + steps for m in range(per_block)], axis=1)
        place_row[...] = places

        def column(row):
            return jnp.broadcast_to(row, (8, BLOCK)).T[:, :1]

        place_col[...] = column(places.astype(jnp.float32)).astype(jnp.int32)
        for n in range(blocks):
            row = jnp.concatenate(
                [sums[pl.ds(n * per_block + (low ^ m), 1), :] for m in range(per_block)], axis=1
            )
            row_ref[n] = row
            col_ref[n] = column(row)

    return kernel(
        body,
        [
            pltpu.VMEM((blocks, 1, BLOCK), jnp.float32),
            pltpu.VMEM((blocks, BLOCK, 1), jnp.float32),
            pltpu.VMEM((blocks, 1), jnp.float32),
            pltpu.VMEM((1, BLOCK), jnp.int32),
            pltpu.VMEM((BLOCK, 1), jnp.int32),
        ],
        [decay_log],
        scalars=ids,
        scratch=[pltpu.VMEM((length // chunk, chunk), jnp.float32)],
    )


def mixed(ids, side, stages, gather):
    steps = len(stages)
    count = len(side)
    split = len(side[0])
    _, piece, width = side[0][0].shape
    chunk = split * piece
    parts = [w.shape[1] for w in stages[0]]
    cuts = [sum(parts[:i]) for i in range(len(parts))]
    length = count * chunk

    def body(ids_ref, *refs):
        turn = turn_of(ids_ref[0] // 2, steps + 1)
        sources = [place_at((turn + steps + 1 - step) % (steps + 1), steps + 1) for step in range(steps + 1)]
        outs = refs[-2:] if gather else refs[-1:]
        first = count * split
        weights = [
            refs[first + step * len(parts) : first + (step + 1) * len(parts)]
            for step in range(steps)
        ]
        for m in range(0, count, 2):

            def rows(step):
                return jnp.concatenate(
                    [ref[sources[step]] for ref in refs[m * split : (m + 2) * split]], axis=0
                )

            span = pl.ds(m * chunk, 2 * chunk)
            for part, cut in enumerate(cuts):
                total = None
                for step in range(steps):
                    product = dot32(rows(step), weights[step][part][...])
                    total = product if total is None else total + product
                outs[0][span, cut : cut + parts[part]] = total
            if gather:
                outs[1][span, :] = rows(steps)

    return kernel(
        body,
        [
            pltpu.VMEM((length, sum(parts)), jnp.float32),
            pltpu.VMEM((length, width), jnp.bfloat16),
        ][: 2 if gather else 1],
        [rows for pieces in side for rows in pieces] + [w for step in stages for w in step],
        scalars=ids,
    )


def projected(total, last, weight, cut, factor):
    (length, _), part = total.shape, weight.shape[1]

    def body(total, last, w, out):
        out[...] = (total[:, cut : cut + part] + dot32(last[...], w[...])) * factor

    return kernel(body, pltpu.VMEM((length, part), jnp.float32), [total, last, weight])


def joined(kept, came, scale):
    return (kept + came.astype(jnp.float32) * (1.0 / scale)).astype(jnp.bfloat16)


def weighed(pair_mine, pair_other, decays, prior, memories):
    log_row, log_col, place_row, place_col = decays
    length, wide = pair_mine.shape
    part = wide // 2
    scaling = (2 * part) ** (-0.5)

    def body(mine, other, log_row, log_col, place_row, place_col, prior, *refs):
        states = refs[: len(memories)]
        out = refs[len(memories)]
        reads = refs[len(memories) + 1 :]

        def scored(ref, rows):
            return lax.dot_general(
                ref[rows, :part],
                ref[:, part:],
                (((1,), (1,)), ((), ())),
                preferred_element_type=jnp.float32,
            )

        tile = min(256, length)
        for start in range(0, length, tile):
            rows = pl.ds(start, tile)
            scores = (scored(mine, rows) + scored(other, rows)) * scaling
            causal = place_col[rows, :] >= place_row[...]
            spread_log = jnp.where(causal, log_col[rows, :] - log_row[...], 0.0)
            out[rows, :] = jnp.where(causal, scores * jnp.exp(spread_log), 0.0).astype(
                jnp.bfloat16
            )
            fade = scaling * jnp.exp(log_col[rows, :] - prior[...])
            for state, read in zip(states, reads):
                total = jnp.zeros((tile, state.shape[1]), jnp.float32)
                for i, ref in enumerate((mine, other)):
                    lead = ref[rows, :part].astype(jnp.float32) * fade
                    total = total + dot_exact(lead, state[i * part : (i + 1) * part, :])
                read[rows, :] = total

    outs = kernel(
        body,
        [pltpu.VMEM((length, length), jnp.bfloat16)]
        + [pltpu.VMEM((length, state.shape[1]), jnp.float32) for state in memories],
        [pair_mine, pair_other, log_row, log_col, place_row, place_col, prior, *memories],
    )
    return outs[0], outs[1:]


def applied(weights, values, carried, gain, chunk):
    length, part = values.shape

    def body(weights_ref, values_ref, carried_ref, gain_ref, *outs):
        for m, out in enumerate(outs):
            rows = pl.ds(m * chunk, chunk)
            out[pl.ds(0, chunk), :] = (
                dot32(weights_ref[rows, :], values_ref[...]) + carried_ref[rows, :]
            )
            out[pl.ds(chunk, TAIL), :] = jnp.broadcast_to(gain_ref[...], (TAIL, part))

    return kernel(
        body,
        [pltpu.VMEM((chunk + TAIL, part), jnp.float32)] * (length // chunk),
        [weights, values, carried, gain],
    )


def finished(ids, pieces):
    count = len(pieces)
    groups = len(pieces[0])
    rows, part = pieces[0][0].shape
    chunk = rows - TAIL
    wide = groups * part

    def body(ids_ref, *refs):
        out = refs[-1]
        for m in range(0, count, 2):
            mine = refs[m * groups : (m + 2) * groups]
            heads = [ref[pl.ds(0, chunk), :] for ref in mine]
            average = jnp.sum(sum(heads), axis=1, keepdims=True) / (2 * wide)
            centered = [head - average for head in heads]
            squares = jnp.sum(sum(c * c for c in centered), axis=1, keepdims=True)
            rate = lax.rsqrt(squares / (2 * wide) + norm_eps)
            for i, c in enumerate(centered):
                which = m + i // groups
                gain = mine[i][pl.ds(chunk, 1), :]
                start = pl.multiple_of((ids_ref[1] ^ which) * wide + i % groups * part, part)
                out[:, pl.ds(start, part)] = (c * rate * gain).astype(jnp.bfloat16)

    return kernel(
        body,
        jax.ShapeDtypeStruct((chunk, count * wide), jnp.bfloat16),
        [ref for piece in pieces for ref in piece],
        scalars=ids,
    )


def whole(tokens, w_query, w_key, w_value, decay_log, group_gain):
    dp = lax.axis_size("dp")
    ctx = lax.axis_size("ctx")
    outer = dp // 2
    chunk = tokens.shape[1]
    width = w_query.shape[0]
    key_part = w_query.shape[1]
    half = w_value.shape[1] // 2
    rank = lax.axis_index("dp")
    me = lax.axis_index("ctx")
    ids = jnp.stack([rank, me]).astype(jnp.int32)
    length = ctx * chunk
    blocks = length // BLOCK
    high = me // (BLOCK // chunk)

    held, away_tokens, own_tokens = prepared(
        ids, tokens[0], w_query, w_key, w_value, outer
    )
    log_rows, log_cols, ends, place_row, place_col = decayed(ids, decay_log[0], chunk)

    order = loop_order(outer)
    ring = [
        (order[i] * 2 + p, order[(i + 1) % outer] * 2 + p) for i in range(outer) for p in range(2)
    ]
    stages = []
    for _ in range(1, outer):
        stages.append(held)
        sent = []
        for piece in held:
            sent.append(lax.ppermute(piece, "dp", ring))
        held = sent

    def rows_of(parts):
        pieces = {0: parts}
        for m in range(2, ctx, 2):
            pieces[m] = []
            for part in parts:
                pieces[m].append(flipped(part, "ctx", m))
        for m in range(0, ctx, 2):
            pieces[m + 1] = []
            for part in pieces[m]:
                pieces[m + 1].append(flipped(part, "ctx", 1))
        return [pieces[m] for m in range(ctx)]

    came = []
    for part in away_tokens:
        came.append(flipped(part, "dp", 1))
    away_rows = rows_of(came)
    own_rows = rows_of(own_tokens)
    early = [[step[0]] for step in stages]
    late = [step[1:] for step in stages]
    away, away_last = mixed(ids, away_rows, early, True)
    kept, kept_last = mixed(ids, own_rows, early, True)
    away_late = mixed(ids, away_rows, late, False)[0]
    kept_late = mixed(ids, own_rows, late, False)[0]

    limit = TOKEN_MOST * WEIGHT_MOST * outer * width
    scale = 2.0 ** math.floor(math.log2(65504.0 / limit))
    stays = []
    for part, weight in enumerate(held):
        cut = max(part - 1, 0) * half
        gone = projected(away_late if part else away, away_last, weight, cut, scale)
        stay = projected(kept_late if part else kept, kept_last, weight, cut, 1.0)
        stays.append((stay, flipped(gone.astype(jnp.float16), "dp", 1)))

    pair_mine = joined(*stays[0], scale)
    chunks = [pair_mine[m * chunk : (m + 1) * chunk] for m in range(ctx)]
    pair_other = flipped(jnp.concatenate([chunks[m ^ 1] for m in range(ctx)]), "ctx", 1)

    def cut_rows(array, block):
        if blocks == 1:
            return array
        return lax.dynamic_slice_in_dim(array, (block ^ high) * BLOCK, BLOCK, axis=0)

    memories = [jnp.zeros((2 * key_part, half), jnp.float32) for _ in stays[1:]]
    prior = jnp.zeros((1, 1), jnp.float32)
    outputs = [jnp.zeros((length, half), jnp.float32) for _ in stays[1:]]
    arrived = [[] for _ in range(ctx)]
    gains = [group_gain[None, i * half : (i + 1) * half] for i in range(len(stays) - 1)]
    values = []
    for stay in stays[1:]:
        values.append(joined(*stay, scale))
    for n in range(blocks):
        mine, other = cut_rows(pair_mine, n), cut_rows(pair_other, n)
        decays = (log_rows[n], log_cols[n], place_row, place_col)
        weights, carried = weighed(mine, other, decays, prior, memories)
        k_block = jnp.concatenate([mine[:, key_part:], other[:, key_part:]], axis=1)
        end = ends[n : n + 1]
        faded = k_block.astype(jnp.float32) * jnp.exp(end - log_cols[n])
        for group in range(len(values)):
            v_block = cut_rows(values[group], n)
            results = applied(weights, v_block, carried[group], gains[group], chunk)
            memories[group] = jnp.exp(end - prior) * memories[group] + dot_exact(
                faded.T, v_block.astype(jnp.float32)
            )
            if blocks > 1:
                outputs[group] = lax.dynamic_update_slice_in_dim(
                    outputs[group],
                    jnp.concatenate([rows[:chunk] for rows in results]),
                    (n ^ high) * BLOCK,
                    axis=0,
                )
            else:
                outputs[group] = results
        prior = end
    for group, results in enumerate(outputs):
        if blocks > 1:
            below = jnp.broadcast_to(gains[group], (TAIL, half))
            results = [
                jnp.concatenate([results[m * chunk : (m + 1) * chunk], below]) for m in range(ctx)
            ]
        arrived[0].append(results[0])
        for m in range(1, ctx):
            arrived[m].append(flipped(results[m], "ctx", m))
    return finished(ids, arrived)[None]


def solution(mesh):
    in_specs = (
        P("dp", "ctx", None),
        P("dp", "ctx"),
        P("dp", "ctx"),
        P("dp", "ctx"),
        P("dp", None, None),
        P("ctx"),
    )
    out_specs = P("dp", "ctx", None)
    return jax.shard_map(whole, mesh=mesh, in_specs=in_specs, out_specs=out_specs, check_vma=False)
```
